32 devices in a mesh: cell: 16 (over z, y, x), pre: 2 (over core).
Axes of the slice: x: 2, y: 2, z: 4, core: 2. Of those that a mesh axis runs over, the one named last changes fastest.
Arguments:
- v_init: float32 [128, 16, 4096], P(None, None, ('cell', 'pre')), may hold values from -6 to 6
- cotangent: float32 [128, 16, 4096], P(None, None, ('cell', 'pre')), may hold values from -6 to 6
- weights: bfloat16 [4096, 4096], P('cell', 'pre'), may hold values from -2 to 2
- leak: float32 [4096], P(('cell', 'pre')), may hold values from 0.2 to 1.5
- drive: float32 [4096], P(('cell', 'pre')), may hold values from 0.5 to 2
- site: int32 [4096], P(('cell', 'pre')), may hold values from 0 to 127
- parent: int32 [128], replicated, may hold values from 0 to 126, as said below
- axial: float32 [128], replicated, may hold values from 1 to 8
- cap: float32 [128], replicated, may hold values from 2 to 6
- bank: float32 [16, 128], replicated, may hold values from -5 to 5
- sched: int32 [2, 16], replicated, may hold values from 0 to 15
Outputs:
- v_final: float32 [128, 16, 4096], P(None, None, ('cell', 'pre'))
- v_grad: float32 [128, 16, 4096], P(None, None, ('cell', 'pre'))
The draws below stay inside these ranges and needn't reach their ends.
Inputs may be any that keep to these rules, and one draw needn't show every extreme that they name: parent[0] = 0, and for i >= 1 parent[i] < i and i - parent[i] <= 8.
All inputs are finite; a program needn't handle non-finite values.
Results may differ from the reference program's by a relative error of at most 0.0021.
Values may be sent and summed in bfloat16 or wider, within the bound.
A program may use at most 64 MiB of HBM per device.

```python
import math
import jax
import jax.numpy as jnp
from jax import lax

CELL_DEV = 128
NCELL = 4096
COMP = 128
TRIALS = 16
PATTERNS = 16
STEPS = 2
N_CELL = 16
N_PRE = 2


def draw_parent(key, part):
    indices = jnp.arange(COMP, dtype=jnp.int32)
    lowest = jnp.maximum(indices - 8, 0)
    spread = jnp.maximum(indices - lowest, 1)
    raw = jax.random.randint(jax.random.fold_in(key, 11), (COMP,), 0, 1 << 20, dtype=jnp.int32)
    chosen = lowest + raw % spread
    return jnp.where(indices == 0, 0, chosen).astype(jnp.int32)


def touch_ends(drawn, own_key, low, largest):
    longest = drawn.shape.index(max(drawn.shape))
    spots = []
    for shift in (0, 1):
        where = [jax.random.randint(jax.random.fold_in(own_key, axis), (), 0, length) for axis, length in enumerate(drawn.shape)]
        where[longest] = (where[longest] + shift) % drawn.shape[longest]
        spots.append(tuple(where))
    return drawn.at[spots[0]].set(low).at[spots[1]].set(largest)


def with_spikes(result, key, source, target, parts, factor):
    owner, partner = [(jnp.arange(result.shape[position]) // (result.shape[position] // parts)).reshape([-1 if axis == position else 1 for axis in range(result.ndim)]) for position in (source, target)]
    chosen = jax.random.permutation(key, parts)[partner]
    strong = (owner == chosen) | (owner == (partner + parts // 2) % parts)
    return jnp.where(strong, factor * result, result)


def steps_of(rng, dims, cuts, smallest, high):
    loudness = 1.0
    for position, parts in cuts:
        draws = jax.random.uniform(jax.random.fold_in(jax.random.fold_in(rng, 6), position), (parts,), jnp.float32, smallest / len(cuts), high / len(cuts))
        loudness = loudness * jnp.repeat(jnp.exp(draws), dims[position] // parts).reshape((-1,) + (1,) * (len(dims) - 1 - position))
    return loudness


def noise(rng, extent, scale, limit, shards=(), kind=jnp.bfloat16):
    result = jax.random.normal(rng, extent, jnp.float32) * scale
    if len(shards) > 0:
        result = steps_of(rng, extent, shards, -0.22, 0.18) * result
    return jnp.clip(result, min=-limit, max=limit).astype(kind)


def gaussian_with(own_key, dims, deviation, reach, cuts, heavy, kind=jnp.bfloat16):
    array = deviation * jax.random.normal(own_key, dims, jnp.float32)
    if cuts:
        array = array * steps_of(own_key, dims, cuts, -0.22, 0.18)
    return jnp.clip(with_spikes(array, jax.random.fold_in(own_key, 3), *heavy), -reach, reach).astype(kind)


def setup_inputs(seed: int = 0) -> dict:
    arg_keys = jax.random.split(jax.random.key(seed), 12)
    v_init = noise(arg_keys[0], (COMP, TRIALS, NCELL), 1.0, 6.0, ((2, 32),), jnp.float32)
    cotangent = noise(arg_keys[1], (COMP, TRIALS, NCELL), 1.0, 6.0, ((2, 32),), jnp.float32)
    weights = gaussian_with(arg_keys[2], (NCELL, NCELL), (max(NCELL // 256, 1)) ** -0.5, 2.0, ((0, 16), (1, 2)), (0, 1, 16, 2.0))
    leak = jnp.clip(jnp.exp(math.log(1.5) - 2.014903 * jax.random.uniform(arg_keys[3], (NCELL,), jnp.float32) ** steps_of(arg_keys[3], (NCELL,), ((0, 32),), -0.2, 0.2)), 0.2, 1.5)
    drive = jnp.clip(jnp.exp(math.log(2.0) - 1.3862944 * jax.random.uniform(arg_keys[4], (NCELL,), jnp.float32) ** steps_of(arg_keys[4], (NCELL,), ((0, 32),), -0.2, 0.2)), 0.5, 2.0)
    site = touch_ends(jax.random.randint(arg_keys[5], (NCELL,), 0, COMP), jax.random.fold_in(arg_keys[5], 1), 0, COMP - 1).astype(jnp.int32)
    parent = draw_parent(jax.random.fold_in(arg_keys[11], 71), 0)
    axial = jnp.clip(jnp.exp(jax.random.uniform(arg_keys[7], (COMP,), jnp.float32, math.log(1.0), math.log(8.0))), 1.0, 8.0)
    cap = jnp.clip(jnp.exp(jax.random.uniform(arg_keys[8], (COMP,), jnp.float32, math.log(2.0), math.log(6.0))), 2.0, 6.0)
    bank = noise(arg_keys[9], (PATTERNS, COMP), 1.0, 5.0, (), jnp.float32)
    sched = touch_ends(jax.random.randint(arg_keys[10], (STEPS, TRIALS), 0, PATTERNS), jax.random.fold_in(arg_keys[10], 1), 0, PATTERNS - 1).astype(jnp.int32)
    return {"v_init": v_init, "cotangent": cotangent, "weights": weights, "leak": leak, "drive": drive, "site": site, "parent": parent, "axial": axial, "cap": cap, "bank": bank, "sched": sched}


reversal = 1.0

def tree_inverse(parent, axial, cap):
    length = parent.shape[0]
    indices = jnp.arange(length, dtype=jnp.int32)
    onehot = (parent[:, None] == indices[None, :]).astype(jnp.float32)
    ident = jnp.eye(length, dtype=jnp.float32)
    edges = (ident - onehot) * (indices > 0).astype(jnp.float32)[:, None]
    shunt = axial * (indices == 0).astype(jnp.float32)
    system = jnp.diag(cap + shunt) + jnp.dot(edges.T * axial[None, :], edges, precision=lax.Precision.HIGHEST)
    lower = jnp.linalg.cholesky(system)
    factor = lax.linalg.triangular_solve(lower, ident, left_side=True, lower=True)
    return jnp.dot(factor.T, factor, precision=lax.Precision.HIGHEST)

def apply_matrix(matrix, field):
    depth, trials, cells = field.shape
    flat = jnp.dot(matrix, field.reshape(depth, trials * cells), precision=lax.Precision.HIGHEST)
    return flat.reshape(depth, trials, cells)

def to_columns(values):
    return values.reshape(TRIALS, N_CELL, N_PRE, CELL_DEV).transpose(0, 2, 1, 3).reshape(TRIALS, NCELL)

def to_cells(values):
    return values.reshape(TRIALS, N_PRE, N_CELL, CELL_DEV).transpose(0, 2, 1, 3).reshape(TRIALS, NCELL)

def reference(v_init, cotangent, weights, leak, drive, site, parent, axial, cap, bank, sched):
    inverse = tree_inverse(parent, axial, cap)
    comps = jnp.arange(COMP, dtype=jnp.int32)
    mask = (site[None, :] == comps[:, None]).astype(jnp.float32)
    levels = cap[:, None, None] - leak[None, None, :]
    select = (sched[:, :, None] == jnp.arange(PATTERNS, dtype=jnp.int32)[None, None, :]).astype(jnp.float32)
    field = v_init
    saved = []
    for moment in range(STEPS):
        rates = jax.nn.sigmoid(field[0])
        activity = rates.astype(jnp.bfloat16)
        synaptic = lax.dot_general(to_columns(activity).astype(jnp.float32), weights.astype(jnp.float32), (((1,), (1,)), ((), ())), preferred_element_type=jnp.float32)
        pattern = jnp.dot(select[moment], bank, precision=lax.Precision.HIGHEST)
        source = pattern.T[:, :, None] * drive[None, None, :]
        total = levels * field + mask[:, None, :] * synaptic[None] * (reversal - field) + source
        saved.append((field, rates, synaptic))
        field = apply_matrix(inverse, total)
    adjoint = cotangent
    for moment in range(STEPS - 1, -1, -1):
        state, rates, synaptic = saved[moment]
        pulled = apply_matrix(inverse.T, adjoint)
        site_adjoint = jnp.sum(mask[:, None, :] * pulled * (reversal - state), axis=0).astype(jnp.bfloat16)
        returned = to_cells(jnp.dot(site_adjoint.astype(jnp.float32), weights.astype(jnp.float32), preferred_element_type=jnp.float32))
        adjoint = levels * pulled - mask[:, None, :] * synaptic[None] * pulled
        adjoint = adjoint.at[0].add(returned * rates * (1.0 - rates))
    return (field, adjoint)
```

```python
import functools

import jax
import jax.numpy as jnp
from jax import lax
from jax.experimental import pallas as pl
from jax.experimental.pallas import tpu as pltpu
from jax.sharding import PartitionSpec as P

f32 = jnp.float32
bf16 = jnp.bfloat16
reversal = 1.0
reach = 8
sweeps = 20
return_dtype = jnp.float32


def split_rows(x):
    hi = x.astype(bf16)
    lo = (x - hi.astype(f32)).astype(bf16)
    return jnp.concatenate([hi, hi, lo], axis=0)


def split_cols(x):
    hi = x.astype(bf16)
    lo = (x - hi.astype(f32)).astype(bf16)
    return jnp.concatenate([hi, lo, hi], axis=1)


def dot3(left, right):
    return jnp.dot(left, right, preferred_element_type=f32)


def tree_inverse(parent, axial, cap):
    n = parent.shape[1]
    lane = lax.broadcasted_iota(jnp.int32, (1, n), 1)
    shifts = [(n - j) % n for j in range(1, min(reach, n - 1) + 1)]

    def rolled(x, s):
        return pltpu.roll(jnp.broadcast_to(x, (8, n)), s, axis=1)[0:1]

    children = []
    for j, s in enumerate(shifts, 1):
        is_child = (rolled(parent, s) == lane) & (lane + j < n)
        children.append(jnp.where(is_child, 1.0, 0.0))
    root = lane == 0
    base = cap + jnp.where(root, axial, 0.0)

    def sweep(_, x):
        g = axial * x / (x + axial)
        g = jnp.where(root, 0.0, g)
        parts = [m * rolled(g, s) for m, s in zip(children, shifts)]
        while len(parts) > 1:
            parts = [sum(parts[k : k + 2]) for k in range(0, len(parts), 2)]
        return base + parts[0]

    x = lax.fori_loop(0, sweeps, sweep, base)
    d = x + jnp.where(root, 0.0, axial)
    f = jnp.where(root, 0.0, axial / d)
    up = lax.broadcasted_iota(jnp.int32, (n, n), 0)
    across = lax.broadcasted_iota(jnp.int32, (n, n), 1)
    power = jnp.where(jnp.broadcast_to(parent, (n, n)) == up, jnp.broadcast_to(f, (n, n)), 0.0)
    total = jnp.where(up == across, 1.0, 0.0) + power
    power = dot3(split_cols(power), split_rows(power))
    width = 2
    while width < n:
        left = split_cols(power)
        if 2 * width < n:
            both = dot3(left, split_rows(jnp.concatenate([total, power], axis=1)))
            total, power = total + both[:, :n], both[:, n:]
        else:
            total = total + dot3(left, split_rows(total))
        width *= 2
    dinv = jnp.broadcast_to(1.0 / d, (n, n)).T
    return dot3(split_cols(total.T), split_rows(dinv * total))


def kernel(
    C, R,
    v_hbm, cot_hbm, w_hbm, leak_ref, drive_ref, site_ref, parent_ref, axial_ref, cap_ref, bank_ref, sched_ref,
    vout_hbm, gout_hbm,
    v_vm, cot_vm, w_vm, vo_vm, go_vm, B, P1, E,
    pat, rows, act, part_f, got_f, sa, part_b, got_b,
    cell_send, cell_recv, pre_send, pre_recv, local,
):
    a = lax.axis_index("cell")
    b = lax.axis_index("pre")
    n = parent_ref.shape[1]
    T = sched_ref.shape[1]
    L = leak_ref.shape[1]
    MESH = pl.DeviceIdType.MESH
    cells = [lax.rem(a + j, C) for j in range(C)]
    pres = [lax.rem(b + j, R) for j in range(R)]

    first = pltpu.make_async_copy(v_hbm.at[pl.ds(0, T)], v_vm.at[pl.ds(0, T)], local.at[0])
    rest = pltpu.make_async_copy(v_hbm.at[pl.ds(T, (n - 1) * T)], v_vm.at[pl.ds(T, (n - 1) * T)], local.at[1])
    cot_in = pltpu.make_async_copy(cot_hbm, cot_vm, local.at[2])
    w_in = pltpu.make_async_copy(w_hbm, w_vm, local.at[3])
    for c in (first, rest, w_in, cot_in):
        c.start()

    barrier = pltpu.get_barrier_semaphore()
    for j in range(1, C):
        pl.semaphore_signal(barrier, inc=1, device_id=(cells[j], b), device_id_type=MESH)
    for j in range(1, R):
        pl.semaphore_signal(barrier, inc=1, device_id=(a, pres[j]), device_id_type=MESH)
    pl.semaphore_wait(barrier, C - 1 + R - 1)

    def to_cells(phase, source, target):
        copies = []
        for j in range(1, C):
            copies.append(pltpu.make_async_remote_copy(
                src_ref=source(cells[j]), dst_ref=target(j),
                send_sem=cell_send.at[phase, j], recv_sem=cell_recv.at[phase, j],
                device_id=(cells[j], b), device_id_type=MESH))
        for c in copies:
            c.start()
        return copies

    def to_pres(phase, source, target):
        copies = []
        for j in range(1, R):
            copies.append(pltpu.make_async_remote_copy(
                src_ref=source(pres[j]), dst_ref=target(j),
                send_sem=pre_send.at[phase, j], recv_sem=pre_recv.at[phase, j],
                device_id=(a, pres[j]), device_id_type=MESH))
        for c in copies:
            c.start()
        return copies

    sent = []

    def arrived(copies):
        for c in copies:
            c.wait_recv()
        sent.extend(copies)

    def share_activity(moment, rates):
        act[moment, a] = rates.astype(bf16)
        return to_cells(moment, lambda _: act.at[moment, a], lambda j: act.at[moment, a])

    def forward(moment, copies):
        arrived(copies)
        gathered = jnp.concatenate([act[moment, j] for j in range(C)], axis=1)
        partial = lax.dot_general(gathered, w_vm[...], (((1,), (1,)), ((), ())), preferred_element_type=f32)
        for r in range(R):
            part_f[moment, r] = partial[:, r * L : (r + 1) * L]
        return to_pres(moment, lambda r: part_f.at[moment, r], lambda j: got_f.at[moment, j])

    def forward_sum(moment, copies):
        arrived(copies)
        total = part_f[moment, b]
        for j in range(1, R):
            total = total + got_f[moment, j]
        return total

    def share_site(moment, value):
        sa[moment, b] = value.astype(bf16)
        return to_pres(2 + moment, lambda _: sa.at[moment, b], lambda j: sa.at[moment, b])

    def backward(moment, copies):
        arrived(copies)
        gathered = jnp.concatenate([sa[moment, r] for r in range(R)], axis=1)
        partial = jnp.dot(gathered, w_vm[...], preferred_element_type=f32)
        for j in range(C):
            part_b[moment, j] = partial[:, j * L : (j + 1) * L].astype(part_b.dtype)
        return to_cells(2 + moment, lambda q: part_b.at[moment, q], lambda j: got_b.at[moment, j])

    def backward_sum(moment, copies):
        arrived(copies)
        parts = [part_b[moment, a].astype(f32)] + [got_b[moment, j].astype(f32) for j in range(1, C)]
        while len(parts) > 1:
            parts = [sum(parts[k : k + 2]) for k in range(0, len(parts), 2)]
        return parts[0]

    def sigmoid(x):
        return 1.0 / (1.0 + jnp.exp(-x))

    first.wait()
    r0 = sigmoid(v_vm[0:T])
    ag0 = share_activity(0, r0)

    inverse = tree_inverse(parent_ref[...], axial_ref[...], cap_ref[...])
    left = split_cols(inverse)
    cap_col = jnp.broadcast_to(cap_ref[...], (n, n)).T
    levels = cap_col[:, :L] - leak_ref[...]
    drive = drive_ref[...]
    mask = jnp.where(site_ref[...] == lax.broadcasted_iota(jnp.int32, (n, L), 0), 1.0, 0.0)
    inv_site = dot3(left, split_rows(mask))
    inv_root = inv_site[0:1]
    inv_own = jnp.sum(mask * inv_site, axis=0, keepdims=True)
    pat[...] = jnp.zeros_like(pat)
    for moment in range(2):
        for t in range(T):
            pat[pl.ds(moment * T + t, 1)] = bank_ref[pl.ds(sched_ref[moment, t], 1)]
    pattern = pat[...].T

    def strided(t):
        return pl.ds(t, n, stride=T)

    def apply(blocks):
        out = dot3(left, split_rows(jnp.concatenate(blocks, axis=1)))
        return [out[:, k * L : (k + 1) * L] for k in range(len(blocks))]

    V0s, Bs, B0, P1s, Es, U0, U1, Q1, W1, S0 = range(10)

    def at_site(x):
        return jnp.sum(mask * x, axis=0, keepdims=True)

    group = 2 if T % 2 == 0 else 1
    rest.wait()
    for t0 in range(0, T, group):
        totals = []
        for t in range(t0, t0 + group):
            x = v_vm[strided(t)]
            rows[V0s, pl.ds(t, 1)] = at_site(x)
            totals.append(levels * x + pattern[:, t : t + 1] * drive)
        for t, y in zip(range(t0, t0 + group), apply(totals)):
            B[t] = y
            rows[Bs, pl.ds(t, 1)] = at_site(y)
            rows[B0, pl.ds(t, 1)] = y[0:1]
    cot_in.wait()
    for t0 in range(0, T, group):
        for t, y in zip(range(t0, t0 + group), apply([cot_vm[strided(t)] for t in range(t0, t0 + group)])):
            P1[t] = y
            rows[P1s, pl.ds(t, 1)] = at_site(y)

    w_in.wait()
    syn0 = forward_sum(0, forward(0, ag0))
    u0 = syn0 * (reversal - rows[V0s])
    v1_root = rows[B0] + inv_root * u0
    v1_own = rows[Bs] + inv_own * u0
    r1 = sigmoid(v1_root)
    ag1 = share_activity(1, r1)
    rs1 = backward(1, share_site(1, rows[P1s] * (reversal - v1_own)))
    rows[U0] = u0
    rows[S0] = syn0

    for t0 in range(0, T, group):
        for t, y in zip(range(t0, t0 + group), apply([levels * P1[t] for t in range(t0, t0 + group)])):
            E[t] = y
            rows[Es, pl.ds(t, 1)] = at_site(y)

    syn1 = forward_sum(1, forward(1, ag1))
    rows[U1] = syn1 * (reversal - v1_own)
    q1 = syn1 * rows[P1s]
    ret1 = backward_sum(1, rs1)
    w1 = ret1 * r1 * (1.0 - r1)
    rs0 = backward(0, share_site(0, (rows[Es] - inv_own * q1 + inv_root * w1) * (reversal - rows[V0s])))
    rows[Q1] = q1
    rows[W1] = w1

    inv_col = jnp.broadcast_to(inverse[:, 0:1], (n, L))
    for t in range(T):
        pulled = E[t] - inv_site * rows[Q1, pl.ds(t, 1)] + inv_col * rows[W1, pl.ds(t, 1)]
        go_vm[strided(t)] = levels * pulled - mask * rows[S0, pl.ds(t, 1)] * pulled
    g_out = pltpu.make_async_copy(go_vm.at[pl.ds(T, (n - 1) * T)], gout_hbm.at[pl.ds(T, (n - 1) * T)], local.at[4])
    g_out.start()
    for t0 in range(0, T, group):
        totals = []
        for t in range(t0, t0 + group):
            v1 = B[t] + inv_site * rows[U0, pl.ds(t, 1)]
            totals.append(levels * v1 + pattern[:, T + t : T + t + 1] * drive)
        for t, y in zip(range(t0, t0 + group), apply(totals)):
            vo_vm[strided(t)] = y + inv_site * rows[U1, pl.ds(t, 1)]
    v_out = pltpu.make_async_copy(vo_vm, vout_hbm, local.at[5])
    v_out.start()

    ret0 = backward_sum(0, rs0)
    go_vm[0:T] = go_vm[0:T] + ret0 * r0 * (1.0 - r0)
    g_last = pltpu.make_async_copy(go_vm.at[pl.ds(0, T)], gout_hbm.at[pl.ds(0, T)], local.at[6])
    g_last.start()
    for c in sent:
        c.wait_send()
    for c in (g_out, v_out, g_last):
        c.wait()


def body(C, R, v_init, cotangent, weights, leak, drive, site, parent, axial, cap, bank, sched):
    n, T, L = v_init.shape
    flat = (n * T, L)
    anywhere = pl.BlockSpec(memory_space=pl.ANY)
    near = pl.BlockSpec(memory_space=pltpu.VMEM)
    slab = pltpu.VMEM((T, n, L), f32)
    v_final, v_grad = pl.pallas_call(
        functools.partial(kernel, C, R),
        out_shape=(jax.ShapeDtypeStruct(flat, f32),) * 2,
        in_specs=[anywhere] * 3 + [near] * 7 + [pl.BlockSpec(memory_space=pltpu.SMEM)],
        out_specs=(anywhere, anywhere),
        scratch_shapes=[
            pltpu.VMEM(flat, f32), pltpu.VMEM(flat, f32), pltpu.VMEM(weights.shape, bf16),
            pltpu.VMEM(flat, f32), pltpu.VMEM(flat, f32), slab, slab, slab,
            pltpu.VMEM((n, n), f32), pltpu.VMEM((10, T, L), f32),
            pltpu.VMEM((2, C, T, L), bf16),
            pltpu.VMEM((2, R, T, L), f32), pltpu.VMEM((2, R, T, L), f32),
            pltpu.VMEM((2, R, T, L), bf16),
            pltpu.VMEM((2, C, T, L), return_dtype), pltpu.VMEM((2, C, T, L), return_dtype),
            pltpu.SemaphoreType.DMA((4, C)), pltpu.SemaphoreType.DMA((4, C)),
            pltpu.SemaphoreType.DMA((4, R)), pltpu.SemaphoreType.DMA((4, R)),
            pltpu.SemaphoreType.DMA((7,)),
        ],
        compiler_params=pltpu.CompilerParams(collective_id=0, has_side_effects=True),
    )(
        v_init.reshape(flat), cotangent.reshape(flat), weights,
        leak.reshape(1, L), drive.reshape(1, L), site.reshape(1, L),
        parent.reshape(1, n), axial.reshape(1, n), cap.reshape(1, n), bank, sched,
    )
    return v_final.reshape(n, T, L), v_grad.reshape(n, T, L)


def solution(mesh):
    own = P(("cell", "pre"))
    field = P(None, None, ("cell", "pre"))
    in_specs = (field, field, P("cell", "pre"), own, own, own, P(), P(), P(), P(), P())
    sizes = mesh.shape["cell"], mesh.shape["pre"]
    return jax.shard_map(
        functools.partial(body, *sizes), mesh=mesh, in_specs=in_specs, out_specs=(field, field), check_vma=False
    )
```

```python
import functools

import jax
import jax.numpy as jnp
from jax import lax
from jax.experimental import pallas as pl
from jax.experimental.pallas import tpu as pltpu
from jax.sharding import PartitionSpec as P

f32 = jnp.float32
bf16 = jnp.bfloat16
reversal = 1.0
reach = 8
sweeps = 20
return_dtype = jnp.bfloat16


def split_rows(x):
    hi = x.astype(bf16)
    lo = (x - hi.astype(f32)).astype(bf16)
    return jnp.concatenate([hi, hi, lo], axis=0)


def split_cols(x):
    hi = x.astype(bf16)
    lo = (x - hi.astype(f32)).astype(bf16)
    return jnp.concatenate([hi, lo, hi], axis=1)


def dot3(left, right):
    return jnp.dot(left, right, preferred_element_type=f32)


def tree_inverse(parent, axial, cap):
    n = parent.shape[1]
    lane = lax.broadcasted_iota(jnp.int32, (1, n), 1)
    shifts = [(n - j) % n for j in range(1, min(reach, n - 1) + 1)]

    def rolled(x, s):
        return pltpu.roll(jnp.broadcast_to(x, (8, n)), s, axis=1)[0:1]

    children = []
    for j, s in enumerate(shifts, 1):
        is_child = (rolled(parent, s) == lane) & (lane + j < n)
        children.append(jnp.where(is_child, 1.0, 0.0))
    root = lane == 0
    base = cap + jnp.where(root, axial, 0.0)

    def sweep(_, x):
        g = axial * x / (x + axial)
        g = jnp.where(root, 0.0, g)
        parts = [m * rolled(g, s) for m, s in zip(children, shifts)]
        while len(parts) > 1:
            parts = [sum(parts[k : k + 2]) for k in range(0, len(parts), 2)]
        return base + parts[0]

    x = lax.fori_loop(0, sweeps, sweep, base)
    d = x + jnp.where(root, 0.0, axial)
    f = jnp.where(root, 0.0, axial / d)
    up = lax.broadcasted_iota(jnp.int32, (n, n), 0)
    across = lax.broadcasted_iota(jnp.int32, (n, n), 1)
    power = jnp.where(jnp.broadcast_to(parent, (n, n)) == up, jnp.broadcast_to(f, (n, n)), 0.0)
    total = jnp.where(up == across, 1.0, 0.0) + power
    power = dot3(split_cols(power), split_rows(power))
    width = 2
    while width < n:
        left = split_cols(power)
        if 2 * width < n:
            both = dot3(left, split_rows(jnp.concatenate([total, power], axis=1)))
            total, power = total + both[:, :n], both[:, n:]
        else:
            total = total + dot3(left, split_rows(total))
        width *= 2
    dinv = jnp.broadcast_to(1.0 / d, (n, n)).T
    return dot3(split_cols(total.T), split_rows(dinv * total))


def kernel(
    C, R,
    v_hbm, cot_hbm, w_hbm, leak_ref, drive_ref, site_ref, parent_ref, axial_ref, cap_ref, bank_ref, sched_ref,
    vo_vm, go_vm,
    v_vm, cot_vm, w_vm, B, P1, E,
    pat, rows, act, part_f, got_f, sa, part_b, got_b,
    cell_send, cell_recv, pre_send, pre_recv, local,
):
    a = lax.axis_index("cell")
    b = lax.axis_index("pre")
    n = parent_ref.shape[1]
    T = sched_ref.shape[1]
    L = leak_ref.shape[1]
    MESH = pl.DeviceIdType.MESH
    cells = [lax.rem(a + j, C) for j in range(C)]
    pres = [lax.rem(b + j, R) for j in range(R)]
    near_first = sorted(range(1, C), key=lambda j: min(j, C - j))

    first = pltpu.make_async_copy(v_hbm.at[pl.ds(0, T)], v_vm.at[pl.ds(0, T)], local.at[0])
    rest = pltpu.make_async_copy(v_hbm.at[pl.ds(T, (n - 1) * T)], v_vm.at[pl.ds(T, (n - 1) * T)], local.at[1])
    cot_in = pltpu.make_async_copy(cot_hbm, cot_vm, local.at[2])
    w_in = pltpu.make_async_copy(w_hbm, w_vm, local.at[3])
    for c in (first, rest, w_in, cot_in):
        c.start()

    barrier = pltpu.get_barrier_semaphore()
    for j in range(1, C):
        pl.semaphore_signal(barrier, inc=1, device_id=(cells[j], b), device_id_type=MESH)
    for j in range(1, R):
        pl.semaphore_signal(barrier, inc=1, device_id=(a, pres[j]), device_id_type=MESH)

    def to_cells(phase, source, target):
        copies = []
        for j in near_first:
            copies.append(pltpu.make_async_remote_copy(
                src_ref=source(cells[j]), dst_ref=target(j),
                send_sem=cell_send.at[phase, j], recv_sem=cell_recv.at[phase, j],
                device_id=(cells[j], b), device_id_type=MESH))
        for c in copies:
            c.start()
        return copies

    def to_pres(phase, source, target):
        copies = []
        for j in range(1, R):
            copies.append(pltpu.make_async_remote_copy(
                src_ref=source(pres[j]), dst_ref=target(j),
                send_sem=pre_send.at[phase, j], recv_sem=pre_recv.at[phase, j],
                device_id=(a, pres[j]), device_id_type=MESH))
        for c in copies:
            c.start()
        return copies

    sent = []

    def arrived(copies):
        for c in copies:
            c.wait_recv()
        sent.extend(copies)

    def share_activity(moment, rates):
        act[moment, a] = rates.astype(bf16)
        return to_cells(moment, lambda _: act.at[moment, a], lambda j: act.at[moment, a])

    def forward(moment, copies):
        arrived(copies)
        gathered = jnp.concatenate([act[moment, j] for j in range(C)], axis=1)
        partial = lax.dot_general(gathered, w_vm[...], (((1,), (1,)), ((), ())), preferred_element_type=f32)
        for r in range(R):
            part_f[moment, r] = partial[:, r * L : (r + 1) * L]
        return to_pres(moment, lambda r: part_f.at[moment, r], lambda j: got_f.at[moment, j])

    def forward_sum(moment, copies):
        arrived(copies)
        total = part_f[moment, b]
        for j in range(1, R):
            total = total + got_f[moment, j]
        return total

    def share_site(moment, value):
        sa[moment, b] = value.astype(bf16)
        return to_pres(2 + moment, lambda _: sa.at[moment, b], lambda j: sa.at[moment, b])

    def backward(moment, copies):
        arrived(copies)
        gathered = jnp.concatenate([sa[moment, r] for r in range(R)], axis=1)
        partial = jnp.dot(gathered, w_vm[...], preferred_element_type=f32)
        for j in range(C):
            part_b[moment, j] = partial[:, j * L : (j + 1) * L].astype(part_b.dtype)
        return to_cells(2 + moment, lambda q: part_b.at[moment, q], lambda j: got_b.at[moment, j])

    def backward_sum(moment, copies):
        arrived(copies)
        parts = [part_b[moment, a].astype(f32)] + [got_b[moment, j].astype(f32) for j in range(1, C)]
        while len(parts) > 1:
            parts = [sum(parts[k : k + 2]) for k in range(0, len(parts), 2)]
        return parts[0]

    def sigmoid(x):
        return 1.0 / (1.0 + jnp.exp(-x))

    first.wait()
    r0 = sigmoid(v_vm[0:T])
    pl.semaphore_wait(barrier, C - 1 + R - 1)
    ag0 = share_activity(0, r0)

    inverse = tree_inverse(parent_ref[...], axial_ref[...], cap_ref[...])
    left = split_cols(inverse)
    cap_col = jnp.broadcast_to(cap_ref[...], (n, n)).T
    levels = cap_col[:, :L] - leak_ref[...]
    drive = drive_ref[...]
    mask = jnp.where(site_ref[...] == lax.broadcasted_iota(jnp.int32, (n, L), 0), 1.0, 0.0)
    inv_site = dot3(left, split_rows(mask))
    inv_root = inv_site[0:1]
    inv_own = jnp.sum(mask * inv_site, axis=0, keepdims=True)
    pat[...] = jnp.zeros_like(pat)
    for moment in range(2):
        for t in range(T):
            pat[pl.ds(moment * T + t, 1)] = bank_ref[pl.ds(sched_ref[moment, t], 1)]
    pattern = pat[...].T

    def strided(t):
        return pl.ds(t, n, stride=T)

    def apply(blocks):
        out = dot3(left, split_rows(jnp.concatenate(blocks, axis=1)))
        return [out[:, k * L : (k + 1) * L] for k in range(len(blocks))]

    V0s, Bs, B0, P1s, Es, U0, U1, Q1, W1, S0 = range(10)

    def at_site(x):
        return jnp.sum(mask * x, axis=0, keepdims=True)

    group = 2 if T % 2 == 0 else 1
    rest.wait()
    for t0 in range(0, T, group):
        totals = []
        for t in range(t0, t0 + group):
            x = v_vm[strided(t)]
            rows[V0s, pl.ds(t, 1)] = at_site(x)
            totals.append(levels * x + pattern[:, t : t + 1] * drive)
        for t, y in zip(range(t0, t0 + group), apply(totals)):
            B[t] = y
            rows[Bs, pl.ds(t, 1)] = at_site(y)
            rows[B0, pl.ds(t, 1)] = y[0:1]
    cot_in.wait()
    for t0 in range(0, T, group):
        for t, y in zip(range(t0, t0 + group), apply([cot_vm[strided(t)] for t in range(t0, t0 + group)])):
            P1[t] = y
            rows[P1s, pl.ds(t, 1)] = at_site(y)

    w_in.wait()
    syn0 = forward_sum(0, forward(0, ag0))
    u0 = syn0 * (reversal - rows[V0s])
    v1_root = rows[B0] + inv_root * u0
    v1_own = rows[Bs] + inv_own * u0
    r1 = sigmoid(v1_root)
    site1 = share_site(1, rows[P1s] * (reversal - v1_own))
    ag1 = share_activity(1, r1)
    rs1 = backward(1, site1)
    rows[U0] = u0
    rows[S0] = syn0

    swap1 = forward(1, ag1)
    for t0 in range(0, T, group):
        for t, y in zip(range(t0, t0 + group), apply([levels * P1[t] for t in range(t0, t0 + group)])):
            E[t] = y
            rows[Es, pl.ds(t, 1)] = at_site(y)

    syn1 = forward_sum(1, swap1)
    rows[U1] = syn1 * (reversal - v1_own)
    q1 = syn1 * rows[P1s]
    ret1 = backward_sum(1, rs1)
    w1 = ret1 * r1 * (1.0 - r1)
    rs0 = backward(0, share_site(0, (rows[Es] - inv_own * q1 + inv_root * w1) * (reversal - rows[V0s])))
    rows[Q1] = q1
    rows[W1] = w1

    inv_col = jnp.broadcast_to(inverse[:, 0:1], (n, L))
    for t in range(T):
        pulled = E[t] - inv_site * rows[Q1, pl.ds(t, 1)] + inv_col * rows[W1, pl.ds(t, 1)]
        go_vm[strided(t)] = levels * pulled - mask * rows[S0, pl.ds(t, 1)] * pulled
    for t0 in range(0, T, group):
        totals = []
        for t in range(t0, t0 + group):
            v1 = B[t] + inv_site * rows[U0, pl.ds(t, 1)]
            totals.append(levels * v1 + pattern[:, T + t : T + t + 1] * drive)
        for t, y in zip(range(t0, t0 + group), apply(totals)):
            vo_vm[strided(t)] = y + inv_site * rows[U1, pl.ds(t, 1)]

    ret0 = backward_sum(0, rs0)
    go_vm[0:T] = go_vm[0:T] + ret0 * r0 * (1.0 - r0)
    for c in sent:
        c.wait_send()


def write_out(v_ref, g_ref, v_hbm, g_hbm, sems):
    copies = [pltpu.make_async_copy(v_ref, v_hbm, sems.at[0]), pltpu.make_async_copy(g_ref, g_hbm, sems.at[1])]
    for c in copies:
        c.start()
    for c in copies:
        c.wait()


def body(C, R, v_init, cotangent, weights, leak, drive, site, parent, axial, cap, bank, sched):
    n, T, L = v_init.shape
    flat = (n * T, L)
    anywhere = pl.BlockSpec(memory_space=pl.ANY)
    near = pl.BlockSpec(memory_space=pltpu.VMEM)
    slab = pltpu.VMEM((T, n, L), f32)
    held = pl.pallas_call(
        functools.partial(kernel, C, R),
        out_shape=(pltpu.VMEM(flat, f32),) * 2,
        in_specs=[anywhere] * 3 + [near] * 7 + [pl.BlockSpec(memory_space=pltpu.SMEM)],
        out_specs=(near, near),
        scratch_shapes=[
            pltpu.VMEM(flat, f32), pltpu.VMEM(flat, f32), pltpu.VMEM(weights.shape, bf16),
            slab, slab, slab,
            pltpu.VMEM((n, n), f32), pltpu.VMEM((10, T, L), f32),
            pltpu.VMEM((2, C, T, L), bf16),
            pltpu.VMEM((2, R, T, L), f32), pltpu.VMEM((2, R, T, L), f32),
            pltpu.VMEM((2, R, T, L), bf16),
            pltpu.VMEM((2, C, T, L), return_dtype), pltpu.VMEM((2, C, T, L), return_dtype),
            pltpu.SemaphoreType.DMA((4, C)), pltpu.SemaphoreType.DMA((4, C)),
            pltpu.SemaphoreType.DMA((4, R)), pltpu.SemaphoreType.DMA((4, R)),
            pltpu.SemaphoreType.DMA((4,)),
        ],
        compiler_params=pltpu.CompilerParams(collective_id=0, has_side_effects=True),
    )(
        v_init.reshape(flat), cotangent.reshape(flat), weights,
        leak.reshape(1, L), drive.reshape(1, L), site.reshape(1, L),
        parent.reshape(1, n), axial.reshape(1, n), cap.reshape(1, n), bank, sched,
    )
    v_final, v_grad = pl.pallas_call(
        write_out,
        out_shape=(jax.ShapeDtypeStruct(flat, f32),) * 2,
        in_specs=[near] * 2,
        out_specs=(anywhere, anywhere),
        scratch_shapes=[pltpu.SemaphoreType.DMA((2,))],
    )(*[pltpu.with_memory_space_constraint(x, pltpu.VMEM) for x in held])
    return v_final.reshape(n, T, L), v_grad.reshape(n, T, L)


def solution(mesh):
    own = P(("cell", "pre"))
    field = P(None, None, ("cell", "pre"))
    in_specs = (field, field, P("cell", "pre"), own, own, own, P(), P(), P(), P(), P())
    sizes = mesh.shape["cell"], mesh.shape["pre"]
    return jax.shard_map(
        functools.partial(body, *sizes), mesh=mesh, in_specs=in_specs, out_specs=(field, field), check_vma=False
    )
```
